32 devices in a mesh: dp: 4 (over z), seq: 8 (over y, x, core).
Axes of the slice: x: 2, y: 2, z: 4, core: 2. Of those that a mesh axis runs over, the one named last changes fastest.
Arguments:
- queries: bfloat16 [4, 1024, 4096], P('dp', 'seq'), may hold values from -6 to 6
- keys: bfloat16 [4, 1024, 4096], P('dp', 'seq'), may hold values from -6 to 6
- values: bfloat16 [4, 1024, 4096], P('dp', 'seq'), may hold values from -6 to 6
- log_decay: float32 [4, 32, 1024], P('dp', None, 'seq'), may hold values from -1 to 0
- attn_grad: bfloat16 [4, 1024, 4096], P('dp', 'seq'), may hold values from -6 to 6
- norm_gain: float32 [4096], replicated, may hold values from 0.1 to 1.9
- route_ids: int32 [4, 1024, 2], P('dp', 'seq'), may hold values from 0 to 7, all different within a row; in each aligned block of 128 rows (0 to 127, 128 to 255, ..., all dimensions but the last counted through in order) at most 40 rows name the same one
- route_weights: float32 [4, 1024, 2], P('dp', 'seq'), may hold values from 0.2 to 1
- grad_exponent: int32 [32], replicated, may hold values from -2 to 2
- w_in: bfloat16 [8, 4608, 4096], P('seq', 'dp'), may hold values from -0.09375 to 0.09375
- w_out: bfloat16 [8, 4608, 4096], P('seq', 'dp'), may hold values from -0.09375 to 0.09375
Outputs:
- layer_out: bfloat16 [4, 1024, 4096], P('dp', 'seq')
- key_out: bfloat16 [4, 1024, 4096], P('dp', 'seq')
- value_out: bfloat16 [4, 1024, 4096], P('dp', 'seq')
The draws below stay inside these ranges and needn't reach their ends.
Inputs may be any that keep to these rules, and one draw needn't show every extreme that they name: `route_ids`: in each aligned block of 128 tokens (the tokens of one device) no expert is chosen by more than 40 tokens, a bound that some block reaches; a token's 2 choices differ.
All inputs are finite; a program needn't handle non-finite values.
Results may differ from the reference program's by a relative error of at most 0.019.
Values may be sent and summed in bfloat16 or wider, within the bound.
No kernel may reach another device: no remote copies, remote signals or barrier semaphores. Data moves between devices by JAX's collectives and lax.ppermute only.
A program may use at most 320 MiB of HBM per device.

```python
import math
import jax
import jax.numpy as jnp
import numpy as np
from jax import lax

ATTENTION_HEADS = 32
HEAD = 128
D = 4096
FF = 4608
TOP = 2
TOK_DEV = 128
EXPERTS = 8
CAP = 40
SEQUENCE_LENGTH = 1024
BATCH_SEQUENCES = 4
N_DP = 4
N_SEQ = 8


def draw_log_decay(key, part):
    complete_keys = jax.random.split(key, 7)
    slow_share = 0.5
    full_shape = (BATCH_SEQUENCES, ATTENTION_HEADS, SEQUENCE_LENGTH)
    slow_heads = jax.random.uniform(complete_keys[0], (BATCH_SEQUENCES, ATTENTION_HEADS, 1)) < slow_share
    slow_rate = jnp.exp(jax.random.uniform(complete_keys[1], (BATCH_SEQUENCES, ATTENTION_HEADS, 1), minval=jnp.log(0.05), maxval=jnp.log(0.25))) * jnp.log(10.0) / SEQUENCE_LENGTH
    fast_rate = jnp.exp(jax.random.uniform(complete_keys[2], (BATCH_SEQUENCES, ATTENTION_HEADS, 1), minval=jnp.log(1.0 / 50.0), maxval=jnp.log(1.0 / 30.0)))
    stride_frequency = jnp.where(slow_heads, slow_rate, fast_rate)
    blocks = SEQUENCE_LENGTH // TOK_DEV
    accelerator_multiplier = jnp.repeat(jnp.exp(jax.random.uniform(complete_keys[3], (BATCH_SEQUENCES, ATTENTION_HEADS, blocks), minval=jnp.log(0.5), maxval=jnp.log(1.5))), TOK_DEV, axis=2)
    jaggedness = jax.random.uniform(complete_keys[4], full_shape, minval=0.5, maxval=1.5)
    position_indices = jnp.arange(SEQUENCE_LENGTH)
    spike_position = jax.random.randint(complete_keys[5], (BATCH_SEQUENCES, 1, 1, 2), 0, SEQUENCE_LENGTH)
    spike_struck = jnp.any(position_indices[None, None, :, None] == spike_position, axis=-1)
    spike_magnitude = jnp.log(jax.random.uniform(complete_keys[6], (BATCH_SEQUENCES, ATTENTION_HEADS, 1), minval=0.5, maxval=0.8))
    sampled_values = -stride_frequency * accelerator_multiplier * jaggedness + jnp.where(spike_struck, spike_magnitude, 0.0)
    return sampled_values.astype(jnp.float32)


def place_ends(result, rng, least, largest):
    index_at = [jax.random.randint(jax.random.fold_in(rng, axis), (), 0, length) for axis, length in enumerate(result.shape)]
    widest = result.shape.index(max(result.shape))
    neighbour = index_at[:widest] + [(index_at[widest] + 1) % result.shape[widest]] + index_at[widest + 1:]
    return result.at[tuple(index_at)].set(least).at[tuple(neighbour)].set(largest)


def block_scale(key, dims, pieces, least, largest):
    def one(position, blocks):
        steps = jax.random.uniform(jax.random.fold_in(jax.random.fold_in(key, 6), position), (blocks,), jnp.float32, least / len(pieces), largest / len(pieces))
        return jnp.repeat(jnp.exp(steps), dims[position] // blocks).reshape((-1,) + (1,) * (len(dims) - position - 1))

    level = one(*pieces[0])
    for cut in pieces[1:]:
        level = level * one(*cut)
    return level


def assign_block(key, own, number, rows, count, top, most, lean):
    sequence = jax.random.permutation(key, count)
    packed, ordinary = load_shares(count, rows * top, most, lean, True), load_shares(count, rows * top, most, lean, False)
    places = jnp.arange(count)

    def named(lengths, rotation):
        used = int((lengths > 0).sum())
        fixed = max(1, used // 4)
        shifted = fixed + (places - fixed + rotation * (used - fixed)) % max(1, count - fixed)
        return jnp.zeros((count,), jnp.int32).at[sequence[jnp.where(places < fixed, places, shifted)]].set(jnp.asarray(lengths, jnp.int32))

    lengths = jnp.where(number % 4 == 0, named(packed, number // 4), named(ordinary, number - number // 4 - 1))
    mixed = jax.random.permutation(jax.random.fold_in(own, 3), count)
    donor, receiver = mixed[0:count // 2 * 2:2], mixed[1:count // 2 * 2:2]
    room = jnp.minimum(lengths[donor] - 1, most - lengths[receiver]) // 2
    room = jnp.where((donor == sequence[0]) | (receiver == sequence[0]) | (lengths[receiver] == 0), 0, jnp.maximum(room, 0))
    shifted = jax.random.randint(jax.random.fold_in(own, 4), (count // 2,), 0, 1 << 20) % (room + 1)
    lengths = lengths.at[donor].add(-shifted).at[receiver].add(shifted)
    items = jnp.searchsorted(jnp.cumsum(lengths), jnp.arange(rows * top), side="right").astype(jnp.int32)
    grid = items.reshape(top, rows).T
    grid = grid[jax.random.permutation(jax.random.fold_in(own, 1), rows)]
    rotation = jax.random.randint(jax.random.fold_in(own, 2), (rows, 1), 0, top)
    return jnp.take_along_axis(grid, (jnp.arange(top)[None, :] + rotation) % top, axis=1)


def load_shares(number_of, total, bound, lean, full):
    loads = [(1 << 20) // math.isqrt(rank ** lean) + 1 for rank in range(1, number_of + 1)]
    largest = bound if full else min(bound, max(-(-total // number_of), total * loads[0] // sum(loads)))
    least = 1 if total - largest >= number_of - 1 else 0
    counts, spare = [largest] + [least] * (number_of - 1), total - largest - least * (number_of - 1)
    while spare > 0:
        candidates = [i for i in range(1, number_of) if counts[i] < largest] or [i for i in range(1, number_of) if counts[i] < bound]
        mass, budget = sum([loads[i] for i in candidates]), spare
        for i in candidates:
            more = min(bound - counts[i], max(1, budget * loads[i] // mass), spare)
            counts[i] = counts[i] + more
            spare = spare - more
    return np.array(counts)


def normal_values(key, shape, width, reach, pieces=(), kind=jnp.bfloat16):
    values = width * jax.random.normal(key, shape, jnp.float32)
    if pieces:
        values = values * block_scale(key, shape, pieces, -0.22, 0.18)
    return jnp.clip(values, -reach, reach).astype(kind)


def setup_inputs(seed: int = 0) -> dict:
    arg_keys = jax.random.split(jax.random.key(seed), 12)
    queries = normal_values(arg_keys[0], (BATCH_SEQUENCES, SEQUENCE_LENGTH, D), 1.0, 6.0, ((0, 4), (1, 8)))
    keys = normal_values(arg_keys[1], (BATCH_SEQUENCES, SEQUENCE_LENGTH, D), 1.0, 6.0, ((0, 4), (1, 8)))
    values = normal_values(arg_keys[2], (BATCH_SEQUENCES, SEQUENCE_LENGTH, D), 1.0, 6.0, ((0, 4), (1, 8)))
    log_decay = draw_log_decay(jax.random.fold_in(arg_keys[11], 71), 0)
    attn_grad = normal_values(arg_keys[4], (BATCH_SEQUENCES, SEQUENCE_LENGTH, D), 1.0, 6.0, ((0, 4), (1, 8)))
    norm_gain = jnp.clip(1.0 + 0.18 * jax.random.normal(arg_keys[5], (D,), jnp.float32), 0.1, 1.9)
    route_ids_keys = jax.random.split(jax.random.fold_in(arg_keys[6], 1), BATCH_SEQUENCES * SEQUENCE_LENGTH // TOK_DEV)
    route_ids_turns = jax.random.permutation(jax.random.fold_in(arg_keys[6], 3), BATCH_SEQUENCES * SEQUENCE_LENGTH // TOK_DEV)
    route_ids = jax.vmap(lambda own, number: assign_block(jax.random.fold_in(arg_keys[6], 2), own, number, TOK_DEV, EXPERTS, TOP, CAP, 1))(route_ids_keys, route_ids_turns).reshape((BATCH_SEQUENCES, SEQUENCE_LENGTH, TOP))
    route_weights = jnp.clip(jnp.exp(math.log(1.0) - 1.609438 * jax.random.uniform(arg_keys[7], (BATCH_SEQUENCES, SEQUENCE_LENGTH, TOP), jnp.float32) ** block_scale(arg_keys[7], (BATCH_SEQUENCES, SEQUENCE_LENGTH, TOP), ((0, 4), (1, 8)), -0.2, 0.2)), 0.2, 1.0)
    grad_exponent = place_ends(jax.random.randint(arg_keys[8], (ATTENTION_HEADS,), -2, 3), jax.random.fold_in(arg_keys[8], 1), -2, 2).astype(jnp.int32)
    w_in = normal_values(arg_keys[9], (EXPERTS, FF, D), D ** -0.5, 0.09375, ((0, 8), (1, 4)))
    w_out = normal_values(arg_keys[10], (EXPERTS, FF, D), FF ** -0.5, 0.09375, ((0, 8), (1, 4)))
    return {"queries": queries, "keys": keys, "values": values, "log_decay": log_decay, "attn_grad": attn_grad, "norm_gain": norm_gain, "route_ids": route_ids, "route_weights": route_weights, "grad_exponent": grad_exponent, "w_in": w_in, "w_out": w_out}


norm_eps = 1e-06
highest = lax.Precision.HIGHEST

def block_decays(decay_rows):
    running = jnp.cumsum(decay_rows, axis=-1)
    block_total = running[..., -1]
    position_indices = jnp.arange(TOK_DEV)
    lower_mask = position_indices[:, None] >= position_indices[None, :]
    spread = running[..., :, None] - running[..., None, :]
    weight = jnp.where(lower_mask, jnp.exp(jnp.where(lower_mask, spread, 0.0)), 0.0)
    return (running, block_total, weight)

def split_heads(stacked):
    shaped = stacked.reshape(BATCH_SEQUENCES, SEQUENCE_LENGTH // TOK_DEV, TOK_DEV, ATTENTION_HEADS, HEAD)
    return jnp.moveaxis(shaped, 1, 0)

def split_decay(log_decay):
    shaped = log_decay.reshape(BATCH_SEQUENCES, ATTENTION_HEADS, SEQUENCE_LENGTH // TOK_DEV, TOK_DEV)
    return jnp.moveaxis(shaped, 2, 0)

def join_blocks(stacked):
    return jnp.moveaxis(stacked, 0, 1).reshape(BATCH_SEQUENCES, SEQUENCE_LENGTH, ATTENTION_HEADS, HEAD)

def reverse_step(back_state, inputs):
    query_block, grad_block, decay_rows = inputs
    running, block_total, weight = block_decays(decay_rows)
    lifted = query_block.astype(jnp.float32) * jnp.exp(jnp.swapaxes(running, 1, 2))[..., None]
    back_local = jnp.einsum('bthp,bthq->bhpq', lifted, grad_block.astype(jnp.float32), precision=highest)
    new_state = jnp.exp(block_total)[..., None, None] * back_state + back_local
    return (new_state, back_state)

def forward_step(state_in, inputs):
    query_block, key_block, value_block, grad_block, decay_rows, back_in = inputs
    running, block_total, weight = block_decays(decay_rows)
    score_scale = 1.0 / HEAD
    query_wide = query_block.astype(jnp.float32)
    key_wide = key_block.astype(jnp.float32)
    value_wide = value_block.astype(jnp.float32)
    grad_wide = grad_block.astype(jnp.float32)
    head_major = jnp.swapaxes(running, 1, 2)
    tail_decay = jnp.exp(block_total[:, None, :] - head_major)[..., None]
    lead_decay = jnp.exp(head_major)[..., None]
    scores = jnp.einsum('bthp,bshp->bhts', query_wide, key_wide)
    attn_probs = (scores * weight * score_scale).astype(jnp.bfloat16)
    attention = jnp.einsum('bhts,bshp->bthp', attn_probs.astype(jnp.float32), value_wide)
    attention = attention + score_scale * lead_decay * jnp.einsum('bthp,bhpq->bthq', query_wide, state_in, precision=highest)
    local_state = jnp.einsum('bshp,bshq->bhpq', key_wide * tail_decay, value_wide, precision=highest)
    new_state = jnp.exp(block_total)[..., None, None] * state_in + local_state
    grad_probs = (jnp.einsum('bthq,bshq->bhts', grad_wide, value_wide) * weight * score_scale).astype(jnp.bfloat16)
    key_grad = jnp.einsum('bhts,bthp->bshp', grad_probs.astype(jnp.float32), query_wide)
    key_grad = key_grad + score_scale * tail_decay * jnp.einsum('bshq,bhpq->bshp', value_wide, back_in, precision=highest)
    value_grad = jnp.einsum('bhts,bthq->bshq', attn_probs.astype(jnp.float32), grad_wide)
    value_grad = value_grad + score_scale * tail_decay * jnp.einsum('bshp,bhpq->bshq', key_wide, back_in, precision=highest)
    return (new_state, (attention, key_grad, value_grad))

def expert_rows(inputs):
    row_block, weight_in, weight_out = inputs
    slice_width = FF // N_DP
    summed = jnp.zeros((row_block.shape[0], D), jnp.float32)
    for part_index in range(N_DP):
        first_unit = part_index * slice_width
        hidden = jax.nn.silu(lax.dot_general(row_block, weight_in[first_unit:first_unit + slice_width], (((1,), (1,)), ((), ())), preferred_element_type=jnp.float32)).astype(jnp.bfloat16)
        slice_out = jnp.dot(hidden, weight_out[first_unit:first_unit + slice_width], preferred_element_type=jnp.float32).astype(jnp.bfloat16)
        summed = summed + lax.optimization_barrier(slice_out).astype(jnp.float32)
    return summed.astype(jnp.bfloat16)

def reference(queries, keys, values, log_decay, attn_grad, norm_gain, route_ids, route_weights, grad_exponent, w_in, w_out):
    query_blocks = split_heads(queries)
    key_blocks = split_heads(keys)
    value_blocks = split_heads(values)
    grad_blocks = split_heads(attn_grad)
    decay_blocks = split_decay(log_decay)
    zero_state = jnp.zeros((BATCH_SEQUENCES, ATTENTION_HEADS, HEAD, HEAD), jnp.float32)
    unused, back_states = lax.scan(reverse_step, zero_state, (query_blocks, grad_blocks, decay_blocks), reverse=True)
    unused, outputs = lax.scan(forward_step, zero_state, (query_blocks, key_blocks, value_blocks, grad_blocks, decay_blocks, back_states))
    attention, key_grad, value_grad = outputs
    factor = jnp.exp2(grad_exponent.astype(jnp.float32))[:, None]
    attn_out = join_blocks(attention).reshape(BATCH_SEQUENCES, SEQUENCE_LENGTH, D).astype(jnp.bfloat16)
    key_out = (join_blocks(key_grad) * factor).reshape(BATCH_SEQUENCES, SEQUENCE_LENGTH, D).astype(jnp.bfloat16)
    value_out = (join_blocks(value_grad) * factor).reshape(BATCH_SEQUENCES, SEQUENCE_LENGTH, D).astype(jnp.bfloat16)
    attn_wide = attn_out.reshape(BATCH_SEQUENCES * SEQUENCE_LENGTH, D).astype(jnp.float32)
    mean_square = lax.optimization_barrier(jnp.mean(attn_wide * attn_wide, axis=-1, keepdims=True))
    normed = (attn_wide * lax.rsqrt(mean_square + norm_eps) * norm_gain).astype(jnp.bfloat16)
    blocks_count = BATCH_SEQUENCES * N_SEQ
    choice_ids = route_ids.reshape(blocks_count, TOK_DEV * TOP).astype(jnp.int32)
    onehot = (choice_ids[..., None] == jnp.arange(EXPERTS, dtype=jnp.int32)[None, None, :]).astype(jnp.int32)
    counted = jnp.cumsum(onehot, axis=1).astype(jnp.int32)
    slot_index = lax.optimization_barrier(jnp.sum((counted - 1) * onehot, axis=-1)).astype(jnp.int32)
    block_index = jnp.arange(blocks_count, dtype=jnp.int32)[:, None]
    target = ((choice_ids * blocks_count + block_index) * CAP + slot_index).reshape(-1).astype(jnp.int32)
    token_rows = jnp.repeat(normed, TOP, axis=0)
    buffer_rows = jnp.zeros((EXPERTS * blocks_count * CAP, D), jnp.bfloat16).at[target].set(token_rows)
    expert_out = lax.map(expert_rows, (buffer_rows.reshape(EXPERTS, blocks_count * CAP, D), w_in, w_out))
    picked = expert_out.reshape(EXPERTS * blocks_count * CAP, D)[target].reshape(BATCH_SEQUENCES * SEQUENCE_LENGTH, TOP, D)
    mixed_rows = attn_wide + lax.optimization_barrier(jnp.sum(route_weights.reshape(BATCH_SEQUENCES * SEQUENCE_LENGTH, TOP)[..., None] * picked.astype(jnp.float32), axis=1))
    layer_out = mixed_rows.astype(jnp.bfloat16).reshape(BATCH_SEQUENCES, SEQUENCE_LENGTH, D)
    return (layer_out, key_out, value_out)
```

```python
import jax
import jax.numpy as jnp
from jax import lax
from jax.sharding import PartitionSpec as P

ATTENTION_HEADS = 32
HEAD = 128
TOP = 2


norm_eps = 1e-06
highest = lax.Precision.HIGHEST


def swap(a, axis, shift):
    count = lax.axis_size(axis)
    return lax.ppermute(a, axis, [(i, i ^ shift) for i in range(count)])


def exchange(pieces, axis):
    return [pieces[0]] + [swap(pieces[s], axis, s) for s in range(1, len(pieces))]


def natural_order(pieces, me):
    stacked = jnp.stack(pieces)
    return jnp.concatenate(
        [lax.dynamic_index_in_dim(stacked, k ^ me, 0, False) for k in range(len(pieces))], axis=0
    )


def carried_states(local, totals, me, count, backward):
    heads = local.shape[0]
    share = heads // count
    chunks = local.astype(jnp.bfloat16).reshape(count, share, HEAD, HEAD)
    arrived = exchange(
        [lax.dynamic_index_in_dim(chunks, me ^ s, 0, False) for s in range(count)], "seq"
    )
    mine = lax.dynamic_slice_in_dim(totals, me * share, share, 1)
    block = me ^ jnp.arange(count)
    sign = -1 if backward else 1
    order = block * sign
    before = order[None, :] < order[:, None]
    between = before[:, :, None] & (order[None, :, None] < order[None, None, :])
    between = between & (order[None, None, :] < order[:, None, None])
    gap = jnp.sum(jnp.where(between[..., None], mine[None, None], 0.0), axis=2)
    factor = jnp.where(before[..., None], jnp.exp(gap), 0.0)
    outgoing = []
    for r in range(count):
        joined = jnp.zeros((share, HEAD, HEAD), jnp.float32)
        for s in range(count):
            if s != r:
                joined = joined + factor[r, s][:, None, None] * arrived[s].astype(jnp.float32)
        outgoing.append(joined.astype(jnp.bfloat16))
    return natural_order(exchange(outgoing, "seq"), me)


def expert_slice(row_block, weight_in, weight_out):
    hidden = jax.nn.silu(
        lax.dot_general(
            row_block, weight_in, (((1,), (1,)), ((), ())), preferred_element_type=jnp.float32
        )
    ).astype(jnp.bfloat16)
    return jnp.dot(hidden, weight_out, preferred_element_type=jnp.float32).astype(jnp.bfloat16)


def slot_rows(ids, me, experts_total, capacity):
    length = ids.shape[0]
    choice_ids = ids.reshape(length * TOP)
    onehot = (choice_ids[:, None] == jnp.arange(experts_total, dtype=jnp.int32)[None, :]).astype(
        jnp.int32
    )
    slot_index = jnp.sum((jnp.cumsum(onehot, axis=0) - 1) * onehot, axis=-1)
    return ((choice_ids ^ me) * capacity + slot_index).reshape(length, TOP)


def cut(rows, count):
    size = rows.shape[0] // count
    return [rows[s * size : (s + 1) * size] for s in range(count)]


def dispatch(features, target, count):
    rows = jnp.arange(count, dtype=jnp.int32)[:, None]
    taken = sum((rows == target[:, c][None, :]).astype(jnp.bfloat16) for c in range(TOP))
    return jnp.dot(taken, features, preferred_element_type=jnp.float32).astype(jnp.bfloat16)


def mix(returned, target, weights):
    rows = jnp.arange(returned.shape[0], dtype=jnp.int32)[None, :]
    spread = sum(
        jnp.where(rows == target[:, c][:, None], weights[:, c][:, None], 0.0) for c in range(TOP)
    )
    high = lax.reduce_precision(spread, 8, 7)
    low = (spread - high).astype(jnp.bfloat16)
    return jnp.dot(
        high.astype(jnp.bfloat16), returned, preferred_element_type=jnp.float32
    ) + jnp.dot(low, returned, preferred_element_type=jnp.float32)


def on_device(
    queries,
    keys,
    values,
    log_decay,
    attn_grad,
    norm_gain,
    route_ids,
    route_weights,
    grad_exponent,
    w_in,
    w_out,
):
    length = queries.shape[1]
    width = queries.shape[2]
    count = lax.axis_size("seq")
    groups = lax.axis_size("dp")
    me = lax.axis_index("seq")
    near = [1] if groups > 1 else []
    far = list(range(2, groups))
    experts_total = w_in.shape[0] * count
    capacity = max(2, TOP * length * 5 // (4 * experts_total))
    weight_in = w_in[0]
    weight_out = w_out[0]

    query_heads = queries[0].reshape(length, ATTENTION_HEADS, HEAD)
    key_heads = keys[0].reshape(length, ATTENTION_HEADS, HEAD)
    value_heads = values[0].reshape(length, ATTENTION_HEADS, HEAD)
    grad_heads = attn_grad[0].reshape(length, ATTENTION_HEADS, HEAD)
    running = jnp.cumsum(log_decay[0], axis=1)
    block_total = running[:, -1]
    totals = jnp.stack(exchange([block_total] * count, "seq"))
    far_ids = {s: swap(route_ids[0], "dp", s) for s in far}
    far_weights = {s: swap(route_weights[0], "dp", s) for s in far}
    position_indices = jnp.arange(length)
    lower_mask = position_indices[:, None] >= position_indices[None, :]
    spread = running[:, :, None] - running[:, None, :]
    weight = jnp.where(lower_mask, jnp.exp(jnp.where(lower_mask, spread, 0.0)), 0.0)
    head_major = running.T
    tail_decay = jnp.exp(block_total[None, :] - head_major)[..., None]
    lead_decay = jnp.exp(head_major)[..., None]
    score_scale = 1.0 / HEAD
    query_wide = query_heads.astype(jnp.float32)
    key_wide = key_heads.astype(jnp.float32)
    value_wide = value_heads.astype(jnp.float32)
    local_state = jnp.einsum("shp,shq->hpq", key_wide * tail_decay, value_wide, precision=highest)
    state_in = carried_states(local_state, totals, me, count, False)
    scores = jnp.einsum("thp,shp->hts", query_heads, key_heads, preferred_element_type=jnp.float32)
    attn_probs = (scores * weight * score_scale).astype(jnp.bfloat16)
    attention = jnp.einsum(
        "hts,shp->thp", attn_probs, value_heads, preferred_element_type=jnp.float32
    )
    attention = attention + score_scale * lead_decay * jnp.einsum(
        "thp,hpq->thq", query_heads, state_in, preferred_element_type=jnp.float32
    )
    attn_out = attention.reshape(length, width).astype(jnp.bfloat16)
    attn_wide = attn_out.astype(jnp.float32)
    mean_square = jnp.mean(attn_wide * attn_wide, axis=-1, keepdims=True)
    normed = (attn_wide * lax.rsqrt(mean_square + norm_eps) * norm_gain).astype(jnp.bfloat16)

    far_normed = {s: swap(normed, "dp", s) for s in far}
    target = slot_rows(route_ids[0], me, experts_total, capacity)
    far_target = {s: slot_rows(far_ids[s], me, experts_total, capacity) for s in far}
    rows = experts_total * capacity
    own_pieces = exchange(cut(dispatch(normed, target, rows), count), "seq")
    near_pieces = {s: [swap(piece, "dp", s) for piece in own_pieces] for s in near}
    far_out = {}
    for s in far:
        pieces = exchange(cut(dispatch(far_normed[s], far_target[s], rows), count), "seq")
        far_out[s] = expert_slice(jnp.concatenate(pieces), weight_in, weight_out)
    own_out = cut(expert_slice(jnp.concatenate(own_pieces), weight_in, weight_out), count)
    near_back = {}
    for s in near:
        out = expert_slice(jnp.concatenate(near_pieces[s]), weight_in, weight_out)
        near_back[s] = [swap(piece, "dp", s) for piece in cut(out, count)]

    far_mixed = {}
    for s in far:
        back = jnp.concatenate(exchange(cut(far_out[s], count), "seq"))
        far_mixed[s] = swap(mix(back, far_target[s], far_weights[s]).astype(jnp.bfloat16), "dp", s)

    query_back = query_wide * lead_decay
    back_local = jnp.einsum(
        "thp,thq->hpq", query_back, grad_heads.astype(jnp.float32), precision=highest
    )
    back_local, own_pieces[-1] = lax.optimization_barrier((back_local, own_pieces[-1]))
    back_in = carried_states(back_local, totals, me, count, True)

    joined = []
    for k in range(count):
        total = own_out[k].astype(jnp.float32)
        for s in near:
            total = total + near_back[s][k].astype(jnp.float32)
        joined.append(total.astype(jnp.bfloat16))
    back = jnp.concatenate(exchange(joined, "seq"))
    mixed_rows = attn_wide + mix(back, target, route_weights[0])
    for s in far:
        mixed_rows = mixed_rows + far_mixed[s].astype(jnp.float32)
    layer_out = mixed_rows.astype(jnp.bfloat16).reshape(1, length, width)

    grad_probs = (
        jnp.einsum("thq,shq->hts", grad_heads, value_heads, preferred_element_type=jnp.float32)
        * weight
        * score_scale
    ).astype(jnp.bfloat16)
    factor = jnp.exp2(grad_exponent.astype(jnp.float32))[None, :, None]
    key_grad = jnp.einsum(
        "hts,thp->shp", grad_probs, query_heads, preferred_element_type=jnp.float32
    )
    key_grad = key_grad + score_scale * tail_decay * jnp.einsum(
        "shq,hpq->shp", value_heads, back_in, preferred_element_type=jnp.float32
    )
    value_grad = jnp.einsum(
        "hts,thq->shq", attn_probs, grad_heads, preferred_element_type=jnp.float32
    )
    value_grad = value_grad + score_scale * tail_decay * jnp.einsum(
        "shp,hpq->shq", key_heads, back_in, preferred_element_type=jnp.float32
    )
    key_out = (key_grad * factor).reshape(1, length, width).astype(jnp.bfloat16)
    value_out = (value_grad * factor).reshape(1, length, width).astype(jnp.bfloat16)
    return (layer_out, key_out, value_out)


def solution(mesh):
    in_specs = (
        P("dp", "seq", None),
        P("dp", "seq", None),
        P("dp", "seq", None),
        P("dp", None, "seq"),
        P("dp", "seq", None),
        P(),
        P("dp", "seq", None),
        P("dp", "seq", None),
        P(),
        P("seq", "dp", None),
        P("seq", "dp", None),
    )
    out_specs = (P("dp", "seq", None), P("dp", "seq", None), P("dp", "seq", None))
    return jax.shard_map(
        on_device, mesh=mesh, in_specs=in_specs, out_specs=out_specs, check_vma=False
    )
```
